1024 devices in a mesh: dp: 16 (over x_lo, z), expert: 64 (over x_hi, y, core).
Axes of the slice: x: 8 (x_hi: 4, x_lo: 2; x = x_hi * 2 + x_lo), y: 8, z: 8, core: 2. Of those that a mesh axis runs over, the one named last changes fastest.
Arguments:
- tokens: bfloat16 [8192, 4096], P('expert', 'dp'), may hold values from -6 to 6
- grad_out: bfloat16 [8192, 4096], P('expert', 'dp'), may hold values from -6 to 6
- expert_ids: int32 [8192, 2], P('expert'), may hold values from 0 to 63, all different within a row; in each aligned block of 128 rows (0 to 127, 128 to 255, ...) at most 6 rows name the same one
- route_weights: float32 [8192, 2], P('expert'), may hold values from 0.05 to 1
- gate_weight: bfloat16 [64, 4096, 768], P('expert', 'dp'), may hold values from -0.09375 to 0.09375
- up_weight: bfloat16 [64, 4096, 768], P('expert', 'dp'), may hold values from -0.09375 to 0.09375
- down_weight: bfloat16 [64, 768, 4096], P('expert', None, 'dp'), may hold values from -0.21875 to 0.21875
Outputs:
- mixed: bfloat16 [8192, 4096], P('expert', 'dp')
- grad_tokens: bfloat16 [8192, 4096], P('expert', 'dp')
- grad_route: float32 [8192, 2], P('expert')
- grad_gate: bfloat16 [64, 4096, 768], P('expert', 'dp')
- grad_up: bfloat16 [64, 4096, 768], P('expert', 'dp')
- grad_down: bfloat16 [64, 768, 4096], P('expert', None, 'dp')
The draws below stay inside these ranges and needn't reach their ends.
Inputs may be any that keep to these rules, and one draw needn't show every extreme that they name: `expert_ids`: each token names 2 different experts; in each aligned block of 128 tokens (the tokens held by each position along `expert`) no expert is named by more than 6 tokens, a bound that some block reaches.
All inputs are finite; a program needn't handle non-finite values.
Results may differ from the reference program's by a relative error of at most 0.029.
Values may be sent and summed in bfloat16 or wider, within the bound.
A program may use at most 32 MiB of HBM per device.

```python
import math
import jax
import jax.numpy as jnp
import numpy as np
from jax import lax

D = 4096
H = 768
TOK_DEV = 128
EXPERTS = 64
TOP = 2
CAP = 6
TOKENS = 8192
N_DP = 16
N_EXPERT = 64


def block_levels(own_key, extent, split, low, largest):
    loudness, own = 1.0, jax.random.fold_in(own_key, 6)
    for dim, shards_of in split:
        steps = jnp.exp(jax.random.uniform(jax.random.fold_in(own, dim), (shards_of,), jnp.float32, low / len(split), largest / len(split)))
        loudness = loudness * jnp.repeat(steps, extent[dim] // shards_of).reshape([-1 if axis == dim else 1 for axis in range(len(extent))])
    return loudness


def deal_out(stream_key, own, number, rows, number_of, top, most, slope):
    order = jax.random.permutation(stream_key, number_of)
    packed, usual = portions_of(number_of, rows * top, most, slope, True), portions_of(number_of, rows * top, most, slope, False)
    places = jnp.arange(number_of)

    def named(lengths, offset_by):
        used = int((lengths > 0).sum())
        fixed = max(1, used // 4)
        shifted = fixed + (places - fixed + offset_by * (used - fixed)) % max(1, number_of - fixed)
        return jnp.zeros((number_of,), jnp.int32).at[order[jnp.where(places < fixed, places, shifted)]].set(jnp.asarray(lengths, jnp.int32))

    lengths = jnp.where(number % 4 == 0, named(packed, number // 4), named(usual, number - number // 4 - 1))
    mixed = jax.random.permutation(jax.random.fold_in(own, 3), number_of)
    source_of, receiver = mixed[0:number_of // 2 * 2:2], mixed[1:number_of // 2 * 2:2]
    room = jnp.minimum(lengths[source_of] - 1, most - lengths[receiver]) // 2
    room = jnp.where((source_of == order[0]) | (receiver == order[0]) | (lengths[receiver] == 0), 0, jnp.maximum(room, 0))
    shifted = jax.random.randint(jax.random.fold_in(own, 4), (number_of // 2,), 0, 1 << 20) % (room + 1)
    lengths = lengths.at[source_of].add(-shifted).at[receiver].add(shifted)
    labels = jnp.searchsorted(jnp.cumsum(lengths), jnp.arange(rows * top), side="right").astype(jnp.int32)
    listing = labels.reshape(top, rows).T
    listing = listing[jax.random.permutation(jax.random.fold_in(own, 1), rows)]
    offset_by = jax.random.randint(jax.random.fold_in(own, 2), (rows, 1), 0, top)
    return jnp.take_along_axis(listing, (jnp.arange(top)[None, :] + offset_by) % top, axis=1)


def portions_of(count, total, limit, skew, full):
    weights = [(1 << 20) // math.isqrt(standing ** skew) + 1 for standing in range(1, count + 1)]
    largest = limit if full else min(limit, max(-(-total // count), total * weights[0] // sum(weights)))
    least = 1 if total - largest >= count - 1 else 0
    holding, rest = [largest] + [least] * (count - 1), total - largest - least * (count - 1)
    while rest > 0:
        free = [i for i in range(1, count) if holding[i] < largest] or [i for i in range(1, count) if holding[i] < limit]
        pool, left = sum([weights[i] for i in free]), rest
        for i in free:
            extra = min(limit - holding[i], max(1, left * weights[i] // pool), rest)
            holding[i] = holding[i] + extra
            rest = rest - extra
    return np.array(holding)


def gaussian(own_key, shape, scale, reach, pieces=(), kind=jnp.bfloat16):
    entries = jax.random.normal(own_key, shape, jnp.float32) * scale
    if len(pieces) > 0:
        entries = block_levels(own_key, shape, pieces, -0.22, 0.18) * entries
    return jnp.clip(entries, min=-reach, max=reach).astype(kind)


def setup_inputs(seed: int = 0) -> dict:
    key_list = jax.random.split(jax.random.key(seed), 8)
    tokens = gaussian(key_list[0], (TOKENS, D), 1.0, 6.0, ((0, 64), (1, 16)))
    grad_out = gaussian(key_list[1], (TOKENS, D), 1.0, 6.0, ((0, 64), (1, 16)))
    expert_ids_keys = jax.random.split(jax.random.fold_in(key_list[2], 1), TOKENS // TOK_DEV)
    expert_ids_turns = jax.random.permutation(jax.random.fold_in(key_list[2], 3), TOKENS // TOK_DEV)
    expert_ids = jax.vmap(lambda own, number: deal_out(jax.random.fold_in(key_list[2], 2), own, number, TOK_DEV, EXPERTS, TOP, CAP, 2))(expert_ids_keys, expert_ids_turns).reshape((TOKENS, TOP))
    route_weights = jnp.clip(jnp.exp(math.log(1.0) - 2.9957323 * jax.random.uniform(key_list[3], (TOKENS, TOP), jnp.float32) ** block_levels(key_list[3], (TOKENS, TOP), ((0, 64),), -0.2, 0.2)), 0.05, 1.0)
    gate_weight = gaussian(key_list[4], (EXPERTS, D, H), D ** -0.5, 0.09375, ((0, 64), (1, 16)))
    up_weight = gaussian(key_list[5], (EXPERTS, D, H), D ** -0.5, 0.09375, ((0, 64), (1, 16)))
    down_weight = gaussian(key_list[6], (EXPERTS, H, D), H ** -0.5, 0.21875, ((0, 64), (2, 16)))
    return {"tokens": tokens, "grad_out": grad_out, "expert_ids": expert_ids, "route_weights": route_weights, "gate_weight": gate_weight, "up_weight": up_weight, "down_weight": down_weight}


def block_partial(first_operand, second_operand, pattern):
    partial_value = jnp.einsum(pattern, first_operand.astype(jnp.float32), second_operand.astype(jnp.float32))
    rounded = lax.optimization_barrier(partial_value.astype(jnp.bfloat16))
    return jnp.sum(rounded.astype(jnp.float32), axis=0)


def activate(gate_sum, up_sum, back_sum):
    gate_sigmoid = jax.nn.sigmoid(gate_sum)
    swished = gate_sum * gate_sigmoid
    hidden = (swished * up_sum).astype(jnp.bfloat16)
    gate_grad = (back_sum * up_sum * gate_sigmoid * (1.0 + gate_sum * (1.0 - gate_sigmoid))).astype(jnp.bfloat16)
    up_grad = (back_sum * swished).astype(jnp.bfloat16)
    return hidden, gate_grad, up_grad


def reference(tokens, grad_out, expert_ids, route_weights, gate_weight, up_weight, down_weight):
    capacity = N_EXPERT * CAP
    feature_share = D // N_DP
    flat_ids = expert_ids.reshape(-1).astype(jnp.int32)
    assigned = flat_ids.shape[0]
    onehot = (flat_ids[:, None] == jnp.arange(EXPERTS, dtype=jnp.int32)[None, :]).astype(jnp.int32)
    before = jnp.cumsum(onehot, axis=0) - onehot
    position = jnp.sum(before * onehot, axis=1).astype(jnp.int32)
    slot_index = (flat_ids * capacity + position).astype(jnp.int32)
    owners = jnp.zeros((EXPERTS * capacity,), jnp.int32).at[slot_index].set(jnp.arange(assigned, dtype=jnp.int32) + 1)
    owners = owners.reshape(EXPERTS, capacity)
    flat_weights = route_weights.reshape(-1)

    def expert_pass(inputs):
        expert_owners, w_gate, w_up, w_down = inputs
        filled = expert_owners > 0
        source = jnp.maximum(expert_owners - 1, 0)
        token_index = source // TOP
        expert_rows = jnp.where(filled[:, None], tokens[token_index], jnp.zeros((), jnp.bfloat16))
        scaled = flat_weights[source][:, None] * grad_out[token_index].astype(jnp.float32)
        expert_grads = jnp.where(filled[:, None], scaled, jnp.zeros((), jnp.float32)).astype(jnp.bfloat16)
        row_blocks = expert_rows.reshape(capacity, N_DP, feature_share)
        grad_blocks = expert_grads.reshape(capacity, N_DP, feature_share)
        gate_sum = block_partial(row_blocks, w_gate.reshape(N_DP, feature_share, H), 'rbd,bdh->brh')
        up_sum = block_partial(row_blocks, w_up.reshape(N_DP, feature_share, H), 'rbd,bdh->brh')
        back_sum = block_partial(grad_blocks, w_down.reshape(H, N_DP, feature_share), 'rbd,hbd->brh')
        hidden, gate_grad, up_grad = activate(gate_sum, up_sum, back_sum)
        out_rows = jnp.dot(hidden, w_down, preferred_element_type=jnp.float32).astype(jnp.bfloat16)
        input_rows = (jnp.dot(gate_grad, w_gate.T, preferred_element_type=jnp.float32)
                      + jnp.dot(up_grad, w_up.T, preferred_element_type=jnp.float32)).astype(jnp.bfloat16)
        grad_gate_e = jnp.dot(expert_rows.T, gate_grad, preferred_element_type=jnp.float32).astype(jnp.bfloat16)
        grad_up_e = jnp.dot(expert_rows.T, up_grad, preferred_element_type=jnp.float32).astype(jnp.bfloat16)
        grad_down_e = jnp.dot(hidden.T, expert_grads, preferred_element_type=jnp.float32).astype(jnp.bfloat16)
        return out_rows, input_rows, grad_gate_e, grad_up_e, grad_down_e

    out_all, input_all, grad_gate, grad_up, grad_down = lax.map(expert_pass, (owners, gate_weight, up_weight, down_weight))
    out_assign = out_all.reshape(EXPERTS * capacity, D)[slot_index].reshape(TOKENS, TOP, D)
    input_assign = input_all.reshape(EXPERTS * capacity, D)[slot_index].reshape(TOKENS, TOP, D)
    mixed = jnp.zeros((TOKENS, D), jnp.float32)
    grad_tokens = jnp.zeros((TOKENS, D), jnp.float32)
    grad_columns = []
    grad_float = grad_out.astype(jnp.float32)
    for column in range(TOP):
        out_float = out_assign[:, column].astype(jnp.float32)
        mixed = mixed + route_weights[:, column][:, None] * out_float
        grad_tokens = grad_tokens + input_assign[:, column].astype(jnp.float32)
        grad_columns.append(jnp.sum(grad_float * out_float, axis=1))
    grad_route = jnp.stack(grad_columns, axis=1)
    return (mixed.astype(jnp.bfloat16), grad_tokens.astype(jnp.bfloat16), grad_route,
            grad_gate, grad_up, grad_down)
```

```python
import functools

import jax
import jax.numpy as jnp
from jax import lax
from jax.experimental import pallas as pl
from jax.experimental.pallas import tpu as pltpu
from jax.sharding import PartitionSpec as P

MESH = pl.DeviceIdType.MESH
F32, BF16 = jnp.float32, jnp.bfloat16
PAD = 8


def dot(a, b, ca=1, cb=0):
    return lax.dot_general(a, b, (((ca,), (cb,)), ((), ())), preferred_element_type=F32)


def one_hot(flag):
    return jnp.where(flag, 1.0, 0.0).astype(BF16)


def iota(shape, dim):
    return lax.broadcasted_iota(jnp.int32, shape, dim).astype(F32)


def kernel(
    n_dp, n_expert, capacity,
    tok, go, ids, ids_t, rw, gw_hbm, uw_hbm, dw_hbm,
    mixed, gtok, groute, gg_hbm, gu_hbm, gd_hbm,
    gw, uw, dw, snd, rcv, xr, cr, part, ring_in, ring_out, x_out, x_in, act, rd,
    snd2, rcv2, gg, gu, gd,
    w_sem, a_sem, rs_send, rs_recv, x_sem, ag_send, ag_recv, rd_send, rd_recv, o_sem,
):
    nz = n_dp // 2
    rows = n_expert * capacity
    slab = rows // nz
    per_slab = n_expert // nz
    padded = n_expert * PAD
    half = part.shape[-1]
    feat = tok.shape[1]
    toks = tok.shape[0]
    me_dp, me = lax.axis_index("dp"), lax.axis_index("expert")
    xl, z = me_dp // nz, lax.rem(me_dp, nz)
    ahead = (xl * nz + lax.rem(z + 1, nz), me)
    behind = (xl * nz + lax.rem(z + nz - 1, nz), me)
    partner = ((1 - xl) * nz + z, me)
    toward = (ahead, behind)

    n_core = 2
    n_xh = 4 if n_expert == 64 else 1
    n_y = n_expert // (n_core * n_xh)
    core, y, xh = lax.rem(me, n_core), lax.rem(me // n_core, n_y), me // (n_core * n_y)

    def peer(i):
        d_xh = lax.rem(i, n_xh)
        d_core = lax.rem(i // n_xh, n_core)
        d_y = i // (n_xh * n_core)
        return (
            lax.rem(xh + d_xh, n_xh) * (n_core * n_y)
            + lax.rem(y + d_y, n_y) * n_core
            + lax.rem(core + d_core, n_core)
        )

    loads = [
        pltpu.make_async_copy(gw_hbm, gw, w_sem.at[0]),
        pltpu.make_async_copy(uw_hbm, uw, w_sem.at[1]),
        pltpu.make_async_copy(dw_hbm, dw, w_sem.at[2]),
    ]
    for c in loads:
        c.start()

    barrier = pltpu.get_barrier_semaphore()
    for who in (ahead, behind, partner):
        pl.semaphore_signal(barrier, inc=1, device_id=who, device_id_type=MESH)

    @pl.loop(1, n_expert)
    def _(i):
        pl.semaphore_signal(barrier, inc=1, device_id=(me_dp, peer(i)), device_id_type=MESH)

    expert_row = iota((n_expert, toks), 0)
    hot_t = [jnp.where(ids_t[k : k + 1, :].astype(F32) == expert_row, 1.0, 0.0) for k in range(2)]
    earlier_t = one_hot(iota((toks, toks), 0) < iota((toks, toks), 1))
    before_t = dot((hot_t[0] + hot_t[1]).astype(BF16), earlier_t)
    slot_rows = iota((padded, toks), 0)
    take_t = []
    for k in range(2):
        pos = jnp.sum(before_t * hot_t[k], axis=0, keepdims=True)
        slot = ids_t[k : k + 1, :].astype(F32) * PAD + pos
        take_t.append(one_hot(slot_rows == slot))

    tokens = tok[...]
    grads = go[...].astype(F32)
    p = [rw[:, k : k + 1] for k in range(2)]
    send_x = dot(take_t[0] + take_t[1], tokens)
    send_c = dot(take_t[0], (p[0] * grads).astype(BF16)) + dot(take_t[1], (p[1] * grads).astype(BF16))
    snd[:, :, :feat] = send_x.reshape(n_expert, PAD, feat).astype(BF16)
    snd[:, :, feat:] = send_c.reshape(n_expert, PAD, feat).astype(BF16)

    pl.semaphore_wait(barrier, n_expert - 1 + 3)

    def exchange(src, dst, s):
        @pl.loop(1, n_expert)
        def _(i):
            to = peer(i)
            pltpu.make_async_remote_copy(
                src_ref=src.at[to], dst_ref=dst.at[me],
                send_sem=a_sem.at[2 * s], recv_sem=a_sem.at[2 * s + 1],
                device_id=(me_dp, to), device_id_type=MESH,
            ).start()

        dst[me] = src[me]

    def exchange_all(src, dst, s):
        return pltpu.make_async_remote_copy(
            src_ref=src.at[pl.ds(0, n_expert - 1)], dst_ref=dst.at[pl.ds(0, n_expert - 1)],
            send_sem=a_sem.at[2 * s], recv_sem=a_sem.at[2 * s + 1],
            device_id=partner, device_id_type=MESH,
        )

    exchange(snd, rcv, 0)

    expert_col = iota((toks, n_expert), 1)
    hot = [jnp.where(ids[:, k : k + 1].astype(F32) == expert_col, 1.0, 0.0) for k in range(2)]
    earlier = one_hot(iota((toks, toks), 1) < iota((toks, toks), 0))
    before = dot(earlier, (hot[0] + hot[1]).astype(BF16))
    slot_cols = iota((toks, padded), 1)
    take, take_dot, pos_col = [], [], []
    for k in range(2):
        base = ids[:, k : k + 1].astype(F32) * PAD
        pos_col.append(jnp.sum(before * hot[k], axis=1, keepdims=True))
        take.append(one_hot(slot_cols == base + pos_col[k]))
        take_dot.append(one_hot(slot_cols == base + capacity))

    r_col = iota((rows, 1), 0)
    group = jnp.floor((r_col + 0.5) / capacity)
    shrink = one_hot(iota((rows, padded), 1) == r_col + (PAD - capacity) * group)
    g_col = iota((padded, 1), 0)
    g_group = jnp.floor((g_col + 0.5) / PAD)
    g_left = g_col - PAD * g_group
    g_row = jnp.where(g_left < capacity, capacity * g_group + g_left, -1.0)
    grow = one_hot(iota((padded, rows), 1) == g_row)
    dot_row = jnp.where(g_left == capacity, jnp.floor((g_group + 0.5) / per_slab), -1.0)
    place_dot = one_hot(iota((padded, 16), 1) == dot_row)

    for c in loads:
        c.wait()
    exchange_all(snd, rcv, 0).wait_recv()
    for at, ref in ((0, xr), (feat, cr)):
        arrived = rcv[:, :, at : at + feat].reshape(padded, feat)
        ref[...] = dot(shrink, arrived).astype(BF16)

    for a, value in enumerate(
        (lambda: dot(xr[...], gw[...]), lambda: dot(xr[...], uw[...]), lambda: dot(cr[...], dw[...], 1, 1))
    ):
        full = value().astype(BF16)
        for h in range(2):
            part[h, a] = full[:, h * half : (h + 1) * half].reshape(nz, slab, half)

    long, short = nz // 2, nz // 2 - 1
    hops = ((long, short), (short, long))
    column = (1 - xl, xl)
    sent = []

    def rs_copy(d, o, s, src):
        return pltpu.make_async_remote_copy(
            src_ref=src, dst_ref=ring_in.at[d, o, s],
            send_sem=rs_send.at[d, o, s], recv_sem=rs_recv.at[d, o, s],
            device_id=toward[d], device_id_type=MESH,
        )

    arriving = {}
    for s in range(long):
        for o in range(2):
            for d in range(2):
                length = hops[d][o]
                if s >= length:
                    continue
                far = length - s
                dest = lax.rem(z + far, nz) if d == 0 else lax.rem(z + nz - far, nz)
                if s == 0:
                    src = part.at[column[o], :, dest]
                else:
                    arriving[d, o].wait_recv()
                    ring_out[d, o, s - 1] = (
                        ring_in[d, o, s - 1].astype(F32) + part[column[o], :, dest].astype(F32)
                    ).astype(BF16)
                    src = ring_out.at[d, o, s - 1]
                c = rs_copy(d, o, s, src)
                c.start()
                sent.append(c)
                arriving[d, o] = c

    def total(o):
        value = part[column[o], :, z].astype(F32)
        for d in range(2):
            if hops[d][o]:
                arriving[d, o].wait_recv()
                value = value + ring_in[d, o, hops[d][o] - 1].astype(F32)
        return value

    x_out[...] = total(0).astype(BF16)
    to_partner = pltpu.make_async_remote_copy(
        src_ref=x_out, dst_ref=x_in, send_sem=x_sem.at[0], recv_sem=x_sem.at[1],
        device_id=partner, device_id_type=MESH,
    )
    to_partner.start()
    sent.append(to_partner)
    own = total(1)
    to_partner.wait_recv()
    own = own + x_in[...].astype(F32)

    gate, up, back = own[0], own[1], own[2]
    sig = jax.nn.sigmoid(gate)
    swished = gate * sig
    hidden = swished * up
    act[xl, 0, z] = hidden.astype(BF16)
    act[xl, 1, z] = (back * up * sig * (1.0 + gate * (1.0 - sig))).astype(BF16)
    act[xl, 2, z] = (back * swished).astype(BF16)
    sums = jnp.sum(hidden * back, axis=1, keepdims=True)
    diagonal = iota((slab, 128), 0) == iota((slab, 128), 1)
    rd[xl, z] = jnp.broadcast_to(
        jnp.sum(jnp.where(diagonal, sums, 0.0), axis=0, keepdims=True), (8, 128)
    )

    def pair_of_copies(src_h, src_z, sems, who):
        return (
            pltpu.make_async_remote_copy(
                src_ref=act.at[src_h, :, src_z], dst_ref=act.at[src_h, :, src_z],
                send_sem=ag_send.at[sems], recv_sem=ag_recv.at[sems],
                device_id=who, device_id_type=MESH,
            ),
            pltpu.make_async_remote_copy(
                src_ref=rd.at[src_h, src_z], dst_ref=rd.at[src_h, src_z],
                send_sem=rd_send.at[sems], recv_sem=rd_recv.at[sems],
                device_id=who, device_id_type=MESH,
            ),
        )

    def go_on(copies):
        for c in copies:
            c.start()
            sent.append(c)
        return copies

    def landed(copies):
        for c in copies:
            c.wait_recv()

    ag_column = (xl, 1 - xl)
    swap = go_on(pair_of_copies(xl, z, 4 * nz, partner))
    coming = {}
    for s in range(long):
        for o in range(2):
            for d in range(2):
                if s >= hops[d][o]:
                    continue
                if s == 0:
                    if o == 1 and d == 0:
                        landed(swap)
                    elif o == 1 and not hops[0][1]:
                        landed(swap)
                else:
                    landed(coming[d, o])
                source = lax.rem(z + nz - s, nz) if d == 0 else lax.rem(z + s, nz)
                coming[d, o] = go_on(
                    pair_of_copies(ag_column[o], source, (d * 2 + o) * nz + s, toward[d])
                )
    for key in coming:
        landed(coming[key])

    full = [
        jnp.concatenate([act[h, a].reshape(rows, half) for h in range(2)], axis=1) for a in range(3)
    ]
    hid, g_grad, u_grad = full
    out_rows = dot(hid, dw[...]).astype(BF16)
    in_rows = (dot(g_grad, gw[...], 1, 1) + dot(u_grad, uw[...], 1, 1)).astype(BF16)
    dots = jnp.concatenate([rd[0, j, 0:1, :] + rd[1, j, 0:1, :] for j in range(nz)], axis=0)
    dots = jnp.concatenate([dots, jnp.zeros((16 - nz, 128), F32)], axis=0)
    parts = []
    for _ in range(3):
        piece = dots.astype(BF16)
        parts.append(piece)
        dots = dots - piece.astype(F32)
    placed = [dot(place_dot, piece) for piece in parts]
    width = 2 * feat
    for at, value in ((0, out_rows), (feat, in_rows)):
        spread = dot(grow, value)
        pieces = []
        for c in range(0, feat, 128):
            k = (at + c) // 128
            block = spread[:, c : c + 128]
            pieces.append(block + placed[k] if k < 3 else block)
        spread = jnp.concatenate(pieces, axis=1)
        snd2[:, :, at : at + feat] = spread.reshape(n_expert, PAD, feat).astype(BF16)
    exchange(snd2, rcv2, 1)

    gg[...] = dot(xr[...], g_grad, 0, 0).astype(BF16)
    gu[...] = dot(xr[...], u_grad, 0, 0).astype(BF16)
    gd[...] = dot(hid, cr[...], 0, 0).astype(BF16)
    stores = [
        pltpu.make_async_copy(gg, gg_hbm, o_sem.at[0]),
        pltpu.make_async_copy(gu, gu_hbm, o_sem.at[1]),
        pltpu.make_async_copy(gd, gd_hbm, o_sem.at[2]),
    ]
    for c in stores:
        c.start()
    for c in sent:
        c.wait_send()
    exchange_all(snd, rcv, 0).wait_send()

    exchange_all(snd2, rcv2, 1).wait_recv()
    back_out = rcv2[:, :, :feat].reshape(padded, feat)
    back_in = rcv2[:, :, feat:].reshape(padded, feat)
    mixed[...] = (p[0] * dot(take[0], back_out) + p[1] * dot(take[1], back_out)).astype(BF16)
    gtok[...] = dot(take[0] + take[1], back_in).astype(BF16)
    lane = iota((toks, 128), 1)
    first = (lax.rem(me, per_slab) * capacity).astype(F32)
    cols = []
    for k in range(2):
        low = dot(take_dot[k], back_out)
        high = dot(take_dot[k], back_in[:, :128])
        picked = low[:, :128] + low[:, 128:256] + high
        mine = jnp.where(lane == first + pos_col[k], picked, 0.0)
        cols.append(jnp.sum(mine, axis=1, keepdims=True) / p[k])
    groute[:, 0:1] = cols[0]
    groute[:, 1:2] = cols[1]
    exchange_all(snd2, rcv2, 1).wait_send()
    for c in stores:
        c.wait()


def local(n_dp, n_expert, tokens, grad_out, expert_ids, route_weights, gate_weight, up_weight, down_weight):
    toks, feat = tokens.shape
    top = expert_ids.shape[1]
    hid = gate_weight.shape[2]
    half = hid // 2
    nz = n_dp // 2
    capacity = max(2, 3 * toks * top // (2 * n_expert))
    rows = n_expert * capacity
    slab = rows // nz
    vmem = pl.BlockSpec(memory_space=pltpu.VMEM)
    hbm = pl.BlockSpec(memory_space=pl.ANY)
    block = (3, slab, half)
    width = 2 * feat
    wire = (n_expert, PAD, width)
    dma = pltpu.SemaphoreType.DMA
    out = pl.pallas_call(
        functools.partial(kernel, n_dp, n_expert, capacity),
        out_shape=(
            jax.ShapeDtypeStruct((toks, feat), BF16),
            jax.ShapeDtypeStruct((toks, feat), BF16),
            jax.ShapeDtypeStruct((toks, top), F32),
            jax.ShapeDtypeStruct((feat, hid), BF16),
            jax.ShapeDtypeStruct((feat, hid), BF16),
            jax.ShapeDtypeStruct((hid, feat), BF16),
        ),
        in_specs=[vmem] * 5 + [hbm] * 3,
        out_specs=(vmem, vmem, vmem, hbm, hbm, hbm),
        scratch_shapes=[
            pltpu.VMEM((feat, hid), BF16),
            pltpu.VMEM((feat, hid), BF16),
            pltpu.VMEM((hid, feat), BF16),
            pltpu.VMEM(wire, BF16),
            pltpu.VMEM(wire, BF16),
            pltpu.VMEM((rows, feat), BF16),
            pltpu.VMEM((rows, feat), BF16),
            pltpu.VMEM((2, 3, nz, slab, half), BF16),
            pltpu.VMEM((2, 2, nz // 2, *block), BF16),
            pltpu.VMEM((2, 2, max(1, nz // 2 - 1), *block), BF16),
            pltpu.VMEM(block, BF16),
            pltpu.VMEM(block, BF16),
            pltpu.VMEM((2, 3, nz, slab, half), BF16),
            pltpu.VMEM((2, nz, 8, 128), F32),
            pltpu.VMEM(wire, BF16),
            pltpu.VMEM(wire, BF16),
            pltpu.VMEM((feat, hid), BF16),
            pltpu.VMEM((feat, hid), BF16),
            pltpu.VMEM((hid, feat), BF16),
            dma((3,)),
            dma((4,)),
            dma((2, 2, nz // 2)),
            dma((2, 2, nz // 2)),
            dma((2,)),
            dma((4 * nz + 1,)),
            dma((4 * nz + 1,)),
            dma((4 * nz + 1,)),
            dma((4 * nz + 1,)),
            dma((3,)),
        ],
        compiler_params=pltpu.CompilerParams(
            collective_id=0, has_side_effects=True, vmem_limit_bytes=40 * 1024 * 1024
        ),
        name="routed_layer",
    )(
        tokens, grad_out, expert_ids, expert_ids.T, route_weights,
        gate_weight.reshape(feat, hid), up_weight.reshape(feat, hid), down_weight.reshape(hid, feat),
    )
    mixed, gtok, groute, gg, gu, gd = out
    return mixed, gtok, groute, gg[None], gu[None], gd[None]


def solution(mesh):
    placed = (
        P("expert", "dp"),
        P("expert", "dp"),
        P("expert", None),
        P("expert", None),
        P("expert", "dp", None),
        P("expert", "dp", None),
        P("expert", None, "dp"),
    )
    return jax.shard_map(
        functools.partial(local, mesh.shape["dp"], mesh.shape["expert"]),
        mesh=mesh,
        in_specs=placed,
        out_specs=(
            P("expert", "dp"),
            P("expert", "dp"),
            P("expert", None),
            P("expert", "dp", None),
            P("expert", "dp", None),
            P("expert", None, "dp"),
        ),
        check_vma=False,
    )
```

```python
import functools

import jax
import jax.numpy as jnp
from jax import lax
from jax.experimental import pallas as pl
from jax.experimental.pallas import tpu as pltpu
from jax.sharding import PartitionSpec as P

MESH = pl.DeviceIdType.MESH
F32, BF16 = jnp.float32, jnp.bfloat16
PAD = 8
LANES = 128

GATE_OTHER, GATE_OWN, UP_OWN, BACK_OTHER, BACK_OWN, BACK_LAST = range(6)
SUMS = (
    (False, 0, 3, False, 1),
    (True, 0, 3, False, 0),
    (True, 3, 3, True, 1),
    (False, 6, 2, False, 0),
    (True, 6, 2, False, 0),
    (True, 8, 1, True, 1),
)
HID_OWN, HID_OTHER, GRAD_OWN, GRAD_OTHER = range(4)
GATHERS = ((True, 0, 3, 0), (False, 0, 2, 1), (True, 3, 6, 1), (False, 3, 3, 0))
ACROSS = {HID_OWN: (2, 1), GRAD_OWN: (6, 3)}


def dot(a, b, ca=1, cb=0):
    return lax.dot_general(a, b, (((ca,), (cb,)), ((), ())), preferred_element_type=F32)


def one_hot(flag):
    return jnp.where(flag, 1.0, 0.0).astype(BF16)


def iota(shape, dim):
    return lax.broadcasted_iota(jnp.int32, shape, dim).astype(F32)


def kernel(
    n_dp, n_expert, capacity,
    tok_hbm, go_hbm, ids_hbm, rw_hbm, gw_hbm, uw_hbm, dw_hbm,
    mixed_hbm, gtok_hbm, groute_hbm, gg_hbm, gu_hbm, gd_hbm,
    tok, go, ids, rw, gw, uw, dw,
    snd, rcv, snd_o, rcv_o, snd_i, rcv_i, snd_r, rcv_r, xr, cr,
    mixed, gtok, groute, gg, gu, gd,
    part, ring_in, ring_out, x_in, swap_out, swap_in, act, rd,
    in_sem, out_sem, a_sem, rs_send, rs_recv, x_send, x_recv, swap_send, swap_recv,
    ag_send, ag_recv, cross_send, cross_recv, rd_send, rd_recv, rdx_send, rdx_recv, first_send, first_recv,
):
    nz = n_dp // 2
    rows = n_expert * capacity
    slab = rows // nz
    per_slab = n_expert // nz
    padded = n_expert * PAD
    feat, toks = tok.shape[1], tok.shape[0]
    me_dp, me = lax.axis_index("dp"), lax.axis_index("expert")
    xl, z = me_dp // nz, lax.rem(me_dp, nz)
    ahead = (xl * nz + lax.rem(z + 1, nz), me)
    behind = (xl * nz + lax.rem(z + nz - 1, nz), me)
    partner = ((1 - xl) * nz + z, me)
    toward = (ahead, behind)
    half_of = {True: xl, False: 1 - xl}

    loads = [
        pltpu.make_async_copy(src, dst, in_sem.at[i])
        for i, (src, dst) in enumerate(
            ((ids_hbm, ids), (rw_hbm, rw), (tok_hbm, tok), (go_hbm, go), (gw_hbm, gw), (uw_hbm, uw), (dw_hbm, dw))
        )
    ]
    for c in loads:
        c.start()

    n_core = 2
    n_xh = 4 if n_expert == 64 else 1
    n_y = n_expert // (n_core * n_xh)
    core, y, xh = lax.rem(me, n_core), lax.rem(me // n_core, n_y), me // (n_core * n_y)
    nearby = [
        lax.rem(xh + d_xh, n_xh) * (n_core * n_y) + lax.rem(core + d_core, n_core)
        for d_core in range(n_core)
        for d_xh in range(n_xh)
    ]

    def each_peer(act_on):
        def at(i, skip):
            d_y = n_y // 2 + (1 - 2 * (i % 2)) * ((i + 1) // 2)
            base = lax.rem(y + d_y, n_y) * n_core
            for there in nearby[skip:]:
                act_on(base + there)

        @pl.loop(0, n_y - 1)
        def _(i):
            at(i, 0)

        at(n_y - 1, 1)

    barrier = pltpu.get_barrier_semaphore()
    for who in (ahead, behind, partner):
        pl.semaphore_signal(barrier, inc=1, device_id=who, device_id_type=MESH)
    each_peer(lambda to: pl.semaphore_signal(barrier, inc=1, device_id=(me_dp, to), device_id_type=MESH))

    loads[0].wait()
    loads[1].wait()
    ids_row = ids[...].astype(F32)
    flat = jnp.concatenate([ids_row, rw[...], jnp.zeros((toks - 4, toks), F32)], axis=0)
    turned = flat.T
    expert_row = iota((n_expert, toks), 0)
    hot_t = [jnp.where(ids_row[k : k + 1, :] == expert_row, 1.0, 0.0) for k in range(2)]
    earlier_t = one_hot(iota((toks, toks), 0) < iota((toks, toks), 1))
    before_t = dot((hot_t[0] + hot_t[1]).astype(BF16), earlier_t)
    slot_rows = iota((rows, toks), 0)
    take_t = []
    for k in range(2):
        pos = jnp.sum(before_t * hot_t[k], axis=0, keepdims=True)
        take_t.append(one_hot(slot_rows == ids_row[k : k + 1, :] * capacity + pos))
    p = [turned[:, 2 + k : 3 + k] for k in range(2)]
    blocks = 2 * feat // LANES
    per_group = PAD // 2 if n_expert < PAD else PAD
    height = per_group * capacity
    tall = blocks * height
    packs = blocks * capacity // PAD
    to_row = iota((tall, 1), 0)
    block = jnp.floor((to_row + 0.5) / height)
    inner = to_row - height * block
    which = jnp.floor((inner + 0.5) / capacity)
    target = which * (blocks * capacity) + block * capacity + (inner - capacity * which)
    unpack = one_hot(iota((tall, tall), 1) == target)
    from_row = iota((1, tall), 1)
    block = jnp.floor((from_row + 0.5) / height)
    inner = from_row - height * block
    which = jnp.floor((inner + 0.5) / capacity)
    source = which * (blocks * capacity) + block * capacity + (inner - capacity * which)
    pack = one_hot(iota((tall, tall), 0) == source)
    loads[2].wait()
    loads[3].wait()
    grads = go[...].astype(F32)
    send_x = dot(take_t[0] + take_t[1], tok[...]).astype(BF16)
    send_c = (dot(take_t[0], (p[0] * grads).astype(BF16)) + dot(take_t[1], (p[1] * grads).astype(BF16))).astype(BF16)
    for j in range(n_expert // per_group):
        lo = j * height
        stacked = jnp.concatenate(
            [v[lo : lo + height, c : c + LANES] for v in (send_x, send_c) for c in range(0, feat, LANES)], axis=0
        )
        snd[j * per_group : (j + 1) * per_group] = dot(pack, stacked).reshape(per_group, packs, PAD, LANES).astype(BF16)

    pl.semaphore_wait(barrier, n_expert - 1 + 3)

    def exchange(src, dst, s):
        def send(to):
            pltpu.make_async_remote_copy(
                src_ref=src.at[to], dst_ref=dst.at[me],
                send_sem=a_sem.at[2 * s], recv_sem=a_sem.at[2 * s + 1],
                device_id=(me_dp, to), device_id_type=MESH,
            ).start()

        each_peer(send)
        dst[me] = src[me]

    def exchange_all(src, dst, s):
        return pltpu.make_async_remote_copy(
            src_ref=src.at[pl.ds(0, n_expert - 1)], dst_ref=dst.at[pl.ds(0, n_expert - 1)],
            send_sem=a_sem.at[2 * s], recv_sem=a_sem.at[2 * s + 1],
            device_id=partner, device_id_type=MESH,
        )

    exchange(snd, rcv, 0)
    expert_col = iota((toks, n_expert), 1)
    hot = [jnp.where(turned[:, k : k + 1] == expert_col, 1.0, 0.0) for k in range(2)]
    earlier = one_hot(iota((toks, toks), 1) < iota((toks, toks), 0))
    before = dot(earlier, (hot[0] + hot[1]).astype(BF16))
    slot_cols = iota((toks, padded), 1)
    take, pos_col = [], []
    for k in range(2):
        base = turned[:, k : k + 1] * PAD
        pos_col.append(jnp.sum(before * hot[k], axis=1, keepdims=True))
        take.append(one_hot(slot_cols == base + pos_col[k]))

    g_col = iota((padded, 1), 0)
    g_group = jnp.floor((g_col + 0.5) / PAD)
    g_left = g_col - PAD * g_group
    g_row = jnp.where(g_left < capacity, capacity * g_group + g_left, -1.0)
    grow = one_hot(iota((padded, rows), 1) == g_row)

    long, short = nz // 2, nz // 2 - 1
    offsets = [long] + [sign * d for d in range(short, 0, -1) for sign in (1, -1)] + [0]
    sent = []

    def go_on(src, dst, send_sem, recv_sem, who):
        c = pltpu.make_async_remote_copy(
            src_ref=src, dst_ref=dst, send_sem=send_sem, recv_sem=recv_sem,
            device_id=who, device_id_type=MESH,
        )
        c.start()
        sent.append(c)
        return c

    def at_z(off):
        return lax.rem(z + nz + off, nz)

    x_late, x_seen, ring = {}, set(), {}

    def put_part(a, value):
        full = value.astype(BF16)
        for h in range(2):
            for u in range(3):
                lo = (3 * h + u) * LANES
                part[h, :, 3 * a + u] = full[:, lo : lo + LANES].reshape(nz, slab, LANES)

    def to_other(k):
        _, u0, n, _, _ = SUMS[k]
        for i, off in enumerate(offsets):
            x_late[k, off] = go_on(
                part.at[half_of[False], at_z(off), pl.ds(u0, n)], x_in.at[at_z(off), pl.ds(u0, n)],
                x_send.at[k, i], x_recv.at[k, i], partner,
            )

    def mine(k, off):
        here, u0, n, crossed, _ = SUMS[k]
        value = part[half_of[here], at_z(off), u0 : u0 + n].astype(F32)
        if crossed:
            x_late[k, off].wait_recv()
            value = value + x_in[at_z(off), u0 : u0 + n].astype(F32)
        return value

    def step(k, s):
        here, u0, n, crossed, far_way = SUMS[k]
        for d in range(2):
            length = long if d == far_way else short
            if s >= length:
                continue
            off = (length - s) * (1 - 2 * d)
            key = long if abs(off) == long else off
            units = pl.ds(u0, n)
            if s == 0 and not crossed:
                src = part.at[half_of[here], at_z(off), units]
            else:
                value = mine(k, key)
                if s:
                    ring[k, d].wait_recv()
                    value = value + ring_in[int(here), d, s - 1, u0 : u0 + n].astype(F32)
                ring_out[int(here), d, s, u0 : u0 + n] = value.astype(BF16)
                src = ring_out.at[int(here), d, s, units]
            ring[k, d] = go_on(
                src, ring_in.at[int(here), d, s, units], rs_send.at[k, d, s], rs_recv.at[k, d, s], toward[d]
            )

    def total(k):
        here, u0, n, _, far_way = SUMS[k]
        value = mine(k, 0)
        for d in range(2):
            length = long if d == far_way else short
            if length:
                ring[k, d].wait_recv()
                value = value + ring_in[int(here), d, length - 1, u0 : u0 + n].astype(F32)
        return value

    def swap(k):
        _, u0, n, _, _ = SUMS[k]
        units = pl.ds(u0, n)
        swap_out[u0 : u0 + n] = total(k).astype(BF16)
        return go_on(swap_out.at[units], swap_in.at[units], swap_send.at[k], swap_recv.at[k], partner)

    def swapped(k, c):
        _, u0, n, _, _ = SUMS[k]
        value = total(k)
        c.wait_recv()
        return value + swap_in[u0 : u0 + n].astype(F32)

    exchange_all(snd, rcv, 0).wait_recv()
    for j in range(n_expert // per_group):
        lo = j * height
        stacked = dot(unpack, rcv[j * per_group : (j + 1) * per_group].reshape(tall, LANES)).astype(BF16)
        for i, (ref, c) in enumerate((ref, c) for ref in (xr, cr) for c in range(0, feat, LANES)):
            ref[lo : lo + height, c : c + LANES] = stacked[i * height : (i + 1) * height]
    for c in loads[4:]:
        c.wait()
    put_part(0, dot(xr[...], gw[...]))
    step(GATE_OTHER, 0)
    step(GATE_OWN, 0)
    put_part(1, dot(xr[...], uw[...]))
    to_other(UP_OWN)
    put_part(2, dot(cr[...], dw[...], 1, 1))
    to_other(BACK_LAST)

    plan = (
        (BACK_OTHER, 0), (BACK_OWN, 0), (GATE_OTHER, 1), (UP_OWN, 0), (BACK_LAST, 0), (GATE_OWN, 1),
        (BACK_OTHER, 1), (BACK_OWN, 1), (GATE_OTHER, 2), (UP_OWN, 1), (BACK_LAST, 1), (GATE_OWN, 2),
        (BACK_OTHER, 2), (BACK_OWN, 2), (GATE_OTHER, 3), (UP_OWN, 2), (BACK_LAST, 2), (GATE_OWN, 3),
        (BACK_OTHER, 3), (BACK_OWN, 3), ("swap", GATE_OTHER), (UP_OWN, 3), (BACK_LAST, 3), ("swap", BACK_OTHER),
    )
    swaps = {}
    for what, s in plan:
        if what == "swap":
            swaps[s] = swap(s)
        elif s < long:
            step(what, s)

    gate = swapped(GATE_OWN, swaps[GATE_OTHER])
    up = total(UP_OWN)
    back = jnp.concatenate([swapped(BACK_OWN, swaps[BACK_OTHER]), total(BACK_LAST)], axis=0)
    sig = jax.nn.sigmoid(gate)
    swished = gate * sig
    hidden = swished * up
    act[xl, z, 0:3] = hidden.astype(BF16)
    act[xl, z, 3:6] = (back * up * sig * (1.0 + gate * (1.0 - sig))).astype(BF16)
    act[xl, z, 6:9] = (back * swished).astype(BF16)
    sums = jnp.sum(jnp.sum(hidden * back, axis=0), axis=1, keepdims=True)
    diagonal = iota((slab, LANES), 0) == iota((slab, LANES), 1)
    rd[xl, z] = jnp.broadcast_to(
        jnp.sum(jnp.where(diagonal, sums, 0.0), axis=0, keepdims=True), (8, LANES)
    )

    own, other = half_of[True], half_of[False]
    comes, crossing = {}, {HID_OWN: [], GRAD_OWN: []}

    def ring_send(k, s, d):
        here, u0, n, far_way = GATHERS[k]
        where = at_z(s if d else -s)
        h, units = half_of[here], pl.ds(u0, n)
        both = [
            go_on(act.at[h, where, units], act.at[h, where, units], ag_send.at[k, d, s], ag_recv.at[k, d, s], toward[d])
        ]
        if k == HID_OWN:
            both.append(go_on(rd.at[h, where], rd.at[h, where], rd_send.at[d, s], rd_recv.at[d, s], toward[d]))
        comes[k, d] = both

    def cross(k, s, d):
        where = at_z(s if d else -s)
        u0, n = ACROSS[k]
        units = pl.ds(u0, n)
        j = int(k == GRAD_OWN)
        crossing[k].append(
            go_on(act.at[own, where, units], act.at[own, where, units], cross_send.at[j, d, s], cross_recv.at[j, d, s], partner)
        )
        if k == HID_OWN:
            crossing[k].append(go_on(rd.at[own, where], rd.at[own, where], rdx_send.at[d, s], rdx_recv.at[d, s], partner))

    def ag_step(k, s):
        here, _, _, far_way = GATHERS[k]
        for d in range(2):
            length = long if d == far_way else short
            if s > length or (s == length and not here) or (s and (k, d) not in comes):
                continue
            if s:
                for c in comes[k, d]:
                    c.wait_recv()
            if s < length:
                ring_send(k, s, d)
            if s and here:
                cross(k, s, d)

    def ag_last(k):
        _, _, _, far_way = GATHERS[k]
        for d in range(2):
            if (k, d) in comes:
                for c in comes[k, d]:
                    c.wait_recv()

    firsts = {}

    def first(k, u0, n):
        units = pl.ds(u0, n)
        j = int(k == GRAD_OWN)
        firsts[k] = [
            go_on(act.at[own, z, units], act.at[own, z, units], first_send.at[j], first_recv.at[j], partner)
        ]
        if k == HID_OWN:
            firsts[k].append(go_on(rd.at[own, z], rd.at[own, z], first_send.at[2], first_recv.at[2], partner))

    first(HID_OWN, 0, 3)
    ag_step(HID_OWN, 0)
    first(GRAD_OWN, 3, 6)
    for job in (
        (HID_OWN, 1), "hid", (HID_OTHER, 0), (GRAD_OWN, 0), "grad", (GRAD_OTHER, 0),
        (HID_OWN, 2), (HID_OTHER, 1), (GRAD_OWN, 1), (GRAD_OTHER, 1),
        (HID_OWN, 3), (HID_OTHER, 2), (GRAD_OWN, 2), (GRAD_OTHER, 2),
        (HID_OWN, 4), (HID_OTHER, 3), (GRAD_OWN, 3), (GRAD_OTHER, 3), (GRAD_OWN, 4),
    ):
        if job in ("hid", "grad"):
            for c in firsts[HID_OWN if job == "hid" else GRAD_OWN]:
                c.wait_recv()
        elif job[1] <= long:
            ag_step(*job)
    ag_last(HID_OTHER)
    for c in crossing[HID_OWN]:
        c.wait_recv()

    def whole(a):
        return jnp.concatenate(
            [act[h, :, 3 * a + u].reshape(rows, LANES) for h in range(2) for u in range(3)], axis=1
        )

    hid = whole(0)
    out_rows = dot(hid, dw[...]).astype(BF16)
    for j in range(nz):
        snd_r[j] = rd[0, j, 0:1, :] + rd[1, j, 0:1, :]
    spread = dot(grow, out_rows)
    snd_o[...] = spread.reshape(n_expert, PAD, feat).astype(BF16)
    exchange(snd_o, rcv_o, 2)

    def send_dots(to):
        pltpu.make_async_remote_copy(
            src_ref=snd_r.at[to // per_slab], dst_ref=rcv_r.at[me],
            send_sem=a_sem.at[2], recv_sem=a_sem.at[3],
            device_id=(me_dp, to), device_id_type=MESH,
        ).start()

    each_peer(send_dots)
    rcv_r[me] = snd_r[me // per_slab]
    ag_last(GRAD_OTHER)
    for c in crossing[GRAD_OWN]:
        c.wait_recv()
    g_grad, u_grad = whole(1), whole(2)
    in_rows = (dot(g_grad, gw[...], 1, 1) + dot(u_grad, uw[...], 1, 1)).astype(BF16)
    snd_i[...] = dot(grow, in_rows).reshape(n_expert, PAD, feat).astype(BF16)
    exchange(snd_i, rcv_i, 3)

    gg[...] = dot(xr[...], g_grad, 0, 0).astype(BF16)
    gu[...] = dot(xr[...], u_grad, 0, 0).astype(BF16)
    gd[...] = dot(hid, cr[...], 0, 0).astype(BF16)
    stores = []

    def store(src, dst):
        c = pltpu.make_async_copy(src, dst, out_sem.at[len(stores)])
        c.start()
        stores.append(c)

    store(gg, gg_hbm)
    store(gu, gu_hbm)
    store(gd, gd_hbm)
    for c in sent:
        c.wait_send()
    exchange_all(snd, rcv, 0).wait_send()

    exchange_all(snd_o, rcv_o, 2).wait_recv()
    back_out = rcv_o[...].reshape(padded, feat)
    mixed[...] = (p[0] * dot(take[0], back_out) + p[1] * dot(take[1], back_out)).astype(BF16)
    exchange_all(rcv_r, rcv_r, 1).wait_recv()
    dots = jnp.concatenate([rcv_r[j] for j in range(n_expert)], axis=0)
    high = dots.astype(BF16)
    rest = dots - high.astype(F32)
    middle = rest.astype(BF16)
    low = (rest - middle.astype(F32)).astype(BF16)
    lane = iota((toks, LANES), 1)
    start = (lax.rem(me, per_slab) * capacity).astype(F32)
    cols = []
    for k in range(2):
        from_expert = hot[k].astype(BF16)
        found = dot(from_expert, high) + dot(from_expert, middle) + dot(from_expert, low)
        picked = jnp.where(lane == start + pos_col[k], found, 0.0)
        cols.append(jnp.sum(picked, axis=1, keepdims=True) / p[k])
    groute[...] = jnp.concatenate(cols + [jnp.zeros((toks, toks - 2), F32)], axis=1).T[0:2, :]
    store(mixed, mixed_hbm)
    store(groute, groute_hbm)
    exchange_all(snd_i, rcv_i, 3).wait_recv()
    gtok[...] = dot(take[0] + take[1], rcv_i[...].reshape(padded, feat)).astype(BF16)
    store(gtok, gtok_hbm)
    exchange_all(snd_o, rcv_o, 2).wait_send()
    exchange_all(snd_i, rcv_i, 3).wait_send()
    exchange_all(rcv_r, rcv_r, 1).wait_send()
    for c in stores:
        c.wait()


def put_out(*refs):
    sem = refs[-1]
    n = (len(refs) - 1) // 3
    come = [pltpu.make_async_copy(refs[i], refs[2 * n + i], sem.at[0, i]) for i in range(n)]
    go = [pltpu.make_async_copy(refs[2 * n + i], refs[n + i], sem.at[1, i]) for i in range(n)]
    for c in come:
        c.start()
    for c, d in zip(come, go):
        c.wait()
        d.start()
    for d in go:
        d.wait()


def local(n_dp, n_expert, tokens, grad_out, expert_ids, route_weights, gate_weight, up_weight, down_weight):
    toks, feat = tokens.shape
    top = expert_ids.shape[1]
    hid = gate_weight.shape[2]
    nz = n_dp // 2
    capacity = max(2, 3 * toks * top // (2 * n_expert))
    rows = n_expert * capacity
    slab = rows // nz
    hop = max(1, nz // 2)
    hbm = pl.BlockSpec(memory_space=pltpu.HBM)
    wire = pltpu.VMEM((n_expert, PAD, feat), BF16)
    front = pltpu.VMEM((n_expert, 2 * feat // LANES * capacity // PAD, PAD, LANES), BF16)
    units = (9, slab, LANES)
    dma = pltpu.SemaphoreType.DMA
    shapes = (
        ((toks, feat), BF16),
        ((toks, feat), BF16),
        ((top, toks), F32),
        ((feat, hid), BF16),
        ((feat, hid), BF16),
        ((hid, feat), BF16),
    )
    out = pl.pallas_call(
        functools.partial(kernel, n_dp, n_expert, capacity),
        out_shape=tuple(jax.ShapeDtypeStruct(s, d) for s, d in shapes),
        in_specs=[hbm] * 7,
        out_specs=(hbm,) * 6,
        scratch_shapes=[
            pltpu.VMEM((toks, feat), BF16),
            pltpu.VMEM((toks, feat), BF16),
            pltpu.VMEM((top, toks), jnp.int32),
            pltpu.VMEM((top, toks), F32),
            pltpu.VMEM((feat, hid), BF16),
            pltpu.VMEM((feat, hid), BF16),
            pltpu.VMEM((hid, feat), BF16),
            *[front] * 2,
            *[wire] * 4,
            pltpu.VMEM((nz, 1, LANES), F32),
            pltpu.VMEM((n_expert, 1, LANES), F32),
            pltpu.VMEM((rows, feat), BF16),
            pltpu.VMEM((rows, feat), BF16),
            *[pltpu.VMEM(s, d) for s, d in shapes],
            pltpu.VMEM((2, nz, *units), BF16),
            pltpu.VMEM((2, 2, hop, *units), BF16),
            pltpu.VMEM((2, 2, hop, *units), BF16),
            pltpu.VMEM((nz, *units), BF16),
            pltpu.VMEM(units, BF16),
            pltpu.VMEM(units, BF16),
            pltpu.VMEM((2, nz, *units), BF16),
            pltpu.VMEM((2, nz, 8, LANES), F32),
            dma((7,)),
            dma((6,)),
            dma((8,)),
            dma((6, 2, hop)),
            dma((6, 2, hop)),
            dma((6, nz)),
            dma((6, nz)),
            dma((6,)),
            dma((6,)),
            dma((4, 2, hop)),
            dma((4, 2, hop)),
            dma((2, 2, hop + 1)),
            dma((2, 2, hop + 1)),
            dma((2, hop)),
            dma((2, hop)),
            dma((2, hop + 1)),
            dma((2, hop + 1)),
            dma((3,)),
            dma((3,)),
        ],
        compiler_params=pltpu.CompilerParams(
            collective_id=0, has_side_effects=True
        ),
        name="routed_layer",
    )(
        tokens, grad_out, expert_ids.T, route_weights.T,
        gate_weight.reshape(feat, hid), up_weight.reshape(feat, hid), down_weight.reshape(hid, feat),
    )
    mixed, gtok, groute, gg, gu, gd = pl.pallas_call(
        put_out,
        out_shape=tuple(jax.ShapeDtypeStruct(s, d) for s, d in shapes),
        in_specs=[hbm] * 6,
        out_specs=(hbm,) * 6,
        scratch_shapes=[pltpu.VMEM(s, d) for s, d in shapes] + [dma((2, 6))],
        name="put_out",
    )(*out)
    return mixed, gtok, groute.T, gg[None], gu[None], gd[None]


def solution(mesh):
    placed = (
        P("expert", "dp"),
        P("expert", "dp"),
        P("expert", None),
        P("expert", None),
        P("expert", "dp", None),
        P("expert", "dp", None),
        P("expert", None, "dp"),
    )
    return jax.shard_map(
        functools.partial(local, mesh.shape["dp"], mesh.shape["expert"]),
        mesh=mesh,
        in_specs=placed,
        out_specs=(
            P("expert", "dp"),
            P("expert", "dp"),
            P("expert", None),
            P("expert", "dp", None),
            P("expert", "dp", None),
            P("expert", None, "dp"),
        ),
        check_vma=False,
    )
```

```python
import functools

import jax
import jax.numpy as jnp
from jax import lax
from jax.experimental import pallas as pl
from jax.experimental.pallas import tpu as pltpu
from jax.sharding import PartitionSpec as P

MESH = pl.DeviceIdType.MESH
F32, BF16 = jnp.float32, jnp.bfloat16
PAD = 8
LANES = 128

GATE_OTHER, GATE_OWN, UP_OWN, BACK_OTHER, BACK_OWN, BACK_LAST = range(6)
SUMS = (
    (False, 0, 3, False, 1),
    (True, 0, 3, False, 0),
    (True, 3, 3, True, 1),
    (False, 6, 2, False, 0),
    (True, 6, 2, False, 0),
    (True, 8, 1, True, 1),
)
HID_OWN, HID_OTHER, GRAD_OWN, GRAD_OTHER = range(4)
GATHERS = ((True, 0, 3, 0), (False, 0, 2, 1), (True, 3, 6, 1), (False, 3, 5, 0))
ACROSS = {HID_OWN: (2, 1), GRAD_OWN: (8, 1)}


def dot(a, b, ca=1, cb=0):
    return lax.dot_general(a, b, (((ca,), (cb,)), ((), ())), preferred_element_type=F32)


def one_hot(flag):
    return jnp.where(flag, 1.0, 0.0).astype(BF16)


def iota(shape, dim):
    return lax.broadcasted_iota(jnp.int32, shape, dim).astype(F32)


def kernel(
    n_dp, n_expert, capacity,
    tok_hbm, go_hbm, ids_hbm, rw_hbm, gw_hbm, uw_hbm, dw_hbm,
    mixed_hbm, gtok_hbm, groute_hbm, gg_hbm, gu_hbm, gd_hbm,
    tok, go, ids, rw, gw, uw, dw,
    snd, rcv, snd_o, rcv_o, snd_i, rcv_i, xr, cr,
    mixed, gtok, groute, gg, gu, gd,
    part, ring_in, ring_out, x_in, swap_out, swap_in, act, rd,
    in_sem, out_sem, a_sem, rs_send, rs_recv, x_send, x_recv, swap_send, swap_recv,
    ag_send, ag_recv, cross_send, cross_recv, rd_send, rd_recv, first_send, first_recv,
):
    nz = n_dp // 2
    rows = n_expert * capacity
    slab = rows // nz
    per_slab = n_expert // nz
    padded = n_expert * PAD
    feat, toks = tok.shape[1], tok.shape[0]
    me_dp, me = lax.axis_index("dp"), lax.axis_index("expert")
    xl, z = me_dp // nz, lax.rem(me_dp, nz)
    ahead = (xl * nz + lax.rem(z + 1, nz), me)
    behind = (xl * nz + lax.rem(z + nz - 1, nz), me)
    partner = ((1 - xl) * nz + z, me)
    toward = (ahead, behind)
    half_of = {True: xl, False: 1 - xl}

    loads = [
        pltpu.make_async_copy(src, dst, in_sem.at[i])
        for i, (src, dst) in enumerate(
            ((ids_hbm, ids), (rw_hbm, rw), (tok_hbm, tok), (go_hbm, go), (gw_hbm, gw), (uw_hbm, uw), (dw_hbm, dw))
        )
    ]
    for c in loads:
        c.start()

    n_core = 2
    n_xh = 4 if n_expert == 64 else 1
    n_y = n_expert // (n_core * n_xh)
    core, y, xh = lax.rem(me, n_core), lax.rem(me // n_core, n_y), me // (n_core * n_y)
    nearby = [
        lax.rem(xh + d_xh, n_xh) * (n_core * n_y) + lax.rem(core + d_core, n_core)
        for d_core in range(n_core)
        for d_xh in range(n_xh)
    ]

    def each_peer(act_on):
        def at(i, skip):
            d_y = n_y // 2 + (1 - 2 * (i % 2)) * ((i + 1) // 2)
            base = lax.rem(y + d_y, n_y) * n_core
            for there in nearby[skip:]:
                act_on(base + there)

        @pl.loop(0, n_y - 1)
        def _(i):
            at(i, 0)

        at(n_y - 1, 1)

    barrier = pltpu.get_barrier_semaphore()
    for who in (ahead, behind, partner):
        pl.semaphore_signal(barrier, inc=1, device_id=who, device_id_type=MESH)
    each_peer(lambda to: pl.semaphore_signal(barrier, inc=1, device_id=(me_dp, to), device_id_type=MESH))

    loads[0].wait()
    loads[1].wait()
    ids_row = ids[...].astype(F32)
    flat = jnp.concatenate([ids_row, rw[...], jnp.zeros((toks - 4, toks), F32)], axis=0)
    turned = flat.T
    expert_row = iota((n_expert, toks), 0)
    hot_t = [jnp.where(ids_row[k : k + 1, :] == expert_row, 1.0, 0.0) for k in range(2)]
    earlier_t = one_hot(iota((toks, toks), 0) < iota((toks, toks), 1))
    before_t = dot((hot_t[0] + hot_t[1]).astype(BF16), earlier_t)
    slot_rows = iota((rows, toks), 0)
    take_t = []
    for k in range(2):
        pos = jnp.sum(before_t * hot_t[k], axis=0, keepdims=True)
        take_t.append(one_hot(slot_rows == ids_row[k : k + 1, :] * capacity + pos))
    p = [turned[:, 2 + k : 3 + k] for k in range(2)]
    blocks = 2 * feat // LANES
    per_group = PAD // 2 if n_expert < PAD else PAD
    height = per_group * capacity
    tall = blocks * height
    packs = blocks * capacity // PAD
    to_row = iota((tall, 1), 0)
    block = jnp.floor((to_row + 0.5) / height)
    inner = to_row - height * block
    which = jnp.floor((inner + 0.5) / capacity)
    target = which * (blocks * capacity) + block * capacity + (inner - capacity * which)
    unpack = one_hot(iota((tall, tall), 1) == target)
    from_row = iota((1, tall), 1)
    block = jnp.floor((from_row + 0.5) / height)
    inner = from_row - height * block
    which = jnp.floor((inner + 0.5) / capacity)
    source = which * (blocks * capacity) + block * capacity + (inner - capacity * which)
    pack = one_hot(iota((tall, tall), 0) == source)
    loads[2].wait()
    loads[3].wait()
    grads = go[...].astype(F32)
    send_x = dot(take_t[0] + take_t[1], tok[...]).astype(BF16)
    send_c = (dot(take_t[0], (p[0] * grads).astype(BF16)) + dot(take_t[1], (p[1] * grads).astype(BF16))).astype(BF16)
    for j in range(n_expert // per_group):
        lo = j * height
        stacked = jnp.concatenate(
            [v[lo : lo + height, c : c + LANES] for v in (send_x, send_c) for c in range(0, feat, LANES)], axis=0
        )
        snd[j * per_group : (j + 1) * per_group] = dot(pack, stacked).reshape(per_group, packs, PAD, LANES).astype(BF16)

    pl.semaphore_wait(barrier, n_expert - 1 + 3)

    def exchange(src, dst, s):
        def send(to):
            pltpu.make_async_remote_copy(
                src_ref=src.at[to], dst_ref=dst.at[me],
                send_sem=a_sem.at[2 * s], recv_sem=a_sem.at[2 * s + 1],
                device_id=(me_dp, to), device_id_type=MESH,
            ).start()

        each_peer(send)
        dst[me] = src[me]

    def exchange_all(src, dst, s):
        return pltpu.make_async_remote_copy(
            src_ref=src.at[pl.ds(0, n_expert - 1)], dst_ref=dst.at[pl.ds(0, n_expert - 1)],
            send_sem=a_sem.at[2 * s], recv_sem=a_sem.at[2 * s + 1],
            device_id=partner, device_id_type=MESH,
        )

    exchange(snd, rcv, 0)
    expert_col = iota((toks, n_expert), 1)
    hot = [jnp.where(turned[:, k : k + 1] == expert_col, 1.0, 0.0) for k in range(2)]
    earlier = one_hot(iota((toks, toks), 1) < iota((toks, toks), 0))
    before = dot(earlier, (hot[0] + hot[1]).astype(BF16))
    slot_cols = iota((toks, padded), 1)
    take, take_dot, pos_col = [], [], []
    for k in range(2):
        base = turned[:, k : k + 1] * PAD
        pos_col.append(jnp.sum(before * hot[k], axis=1, keepdims=True))
        take.append(one_hot(slot_cols == base + pos_col[k]))
        take_dot.append(one_hot(slot_cols == base + capacity))

    g_col = iota((padded, 1), 0)
    g_group = jnp.floor((g_col + 0.5) / PAD)
    g_left = g_col - PAD * g_group
    g_row = jnp.where(g_left < capacity, capacity * g_group + g_left, -1.0)
    grow = one_hot(iota((padded, rows), 1) == g_row)
    dot_row = jnp.where(g_left == capacity, jnp.floor((g_group + 0.5) / per_slab), -1.0)
    place_dot = one_hot(iota((padded, 16), 1) == dot_row)

    long, short = nz // 2, nz // 2 - 1
    offsets = [long] + [sign * d for d in range(short, 0, -1) for sign in (1, -1)] + [0]
    sent = []

    waits = {}

    def go_on(src, dst, send_sem, recv_sem, who, once=None):
        c = pltpu.make_async_remote_copy(
            src_ref=src, dst_ref=dst, send_sem=send_sem, recv_sem=recv_sem,
            device_id=who, device_id_type=MESH,
        )
        c.start()
        if once is None:
            sent.append(c)
        else:
            waits[once[0]] = (once[1], send_sem)
        return c

    def all_of(ref, send_sem, recv_sem):
        return pltpu.make_async_remote_copy(
            src_ref=ref, dst_ref=ref, send_sem=send_sem, recv_sem=recv_sem,
            device_id=partner, device_id_type=MESH,
        )

    def at_z(off):
        return lax.rem(z + nz + off, nz)

    x_late, x_seen, ring = {}, set(), {}

    def put_part(a, value):
        full = value.astype(BF16)
        for h in range(2):
            for u in range(3):
                lo = (3 * h + u) * LANES
                part[h, :, 3 * a + u] = full[:, lo : lo + LANES].reshape(nz, slab, LANES)

    def to_other(k):
        _, u0, n, _, _ = SUMS[k]
        for i, off in enumerate(offsets):
            x_late[k, off] = go_on(
                part.at[half_of[False], at_z(off), pl.ds(u0, n)], x_in.at[at_z(off), pl.ds(u0, n)],
                x_send.at[int(k == UP_OWN)], x_recv.at[int(k == UP_OWN), i], partner,
                ("x%d" % k, part.at[0, :, pl.ds(u0, n)]),
            )

    def mine(k, off):
        here, u0, n, crossed, _ = SUMS[k]
        value = part[half_of[here], at_z(off), u0 : u0 + n].astype(F32)
        if crossed:
            x_late[k, off].wait_recv()
            value = value + x_in[at_z(off), u0 : u0 + n].astype(F32)
        return value

    def step(k, s):
        here, u0, n, crossed, far_way = SUMS[k]
        for d in range(2):
            length = long if d == far_way else short
            if s >= length:
                continue
            off = (length - s) * (1 - 2 * d)
            key = long if abs(off) == long else off
            units = pl.ds(u0, n)
            if s == 0 and not crossed:
                src = part.at[half_of[here], at_z(off), units]
            else:
                value = mine(k, key)
                if s:
                    ring[k, d].wait_recv()
                    value = value + ring_in[int(here), d, s - 1, u0 : u0 + n].astype(F32)
                ring_out[int(here), d, s, u0 : u0 + n] = value.astype(BF16)
                src = ring_out.at[int(here), d, s, units]
            ring[k, d] = go_on(
                src, ring_in.at[int(here), d, s, units], rs_send.at[k], rs_recv.at[k, d, s], toward[d],
                ("s%d" % k, part.at[0, pl.ds(0, nz - 1), units]),
            )

    def total(k):
        here, u0, n, _, far_way = SUMS[k]
        value = mine(k, 0)
        for d in range(2):
            length = long if d == far_way else short
            if length:
                ring[k, d].wait_recv()
                value = value + ring_in[int(here), d, length - 1, u0 : u0 + n].astype(F32)
        return value

    def swap(k):
        _, u0, n, _, _ = SUMS[k]
        units = pl.ds(u0, n)
        swap_out[u0 : u0 + n] = total(k).astype(BF16)
        return go_on(swap_out.at[units], swap_in.at[units], swap_send.at[int(k == BACK_OTHER)], swap_recv.at[int(k == BACK_OTHER)], partner)

    def swapped(k, c):
        _, u0, n, _, _ = SUMS[k]
        value = total(k)
        c.wait_recv()
        return value + swap_in[u0 : u0 + n].astype(F32)

    exchange_all(snd, rcv, 0).wait_recv()
    for j in range(n_expert // per_group):
        lo = j * height
        stacked = dot(unpack, rcv[j * per_group : (j + 1) * per_group].reshape(tall, LANES)).astype(BF16)
        for i, (ref, c) in enumerate((ref, c) for ref in (xr, cr) for c in range(0, feat, LANES)):
            ref[lo : lo + height, c : c + LANES] = stacked[i * height : (i + 1) * height]
    for c in loads[4:]:
        c.wait()
    put_part(0, dot(xr[...], gw[...]))
    step(GATE_OTHER, 0)
    step(GATE_OWN, 0)
    put_part(1, dot(xr[...], uw[...]))
    to_other(UP_OWN)
    put_part(2, dot(cr[...], dw[...], 1, 1))
    to_other(BACK_LAST)

    plan = (
        (BACK_OTHER, 0), (BACK_OWN, 0), (GATE_OTHER, 1), (UP_OWN, 0), (BACK_LAST, 0), (GATE_OWN, 1),
        (BACK_OTHER, 1), (BACK_OWN, 1), (GATE_OTHER, 2), (UP_OWN, 1), (BACK_LAST, 1), (GATE_OWN, 2),
        (BACK_OTHER, 2), (BACK_OWN, 2), (GATE_OTHER, 3), (UP_OWN, 2), (BACK_LAST, 2), (GATE_OWN, 3),
        (BACK_OTHER, 3), (BACK_OWN, 3), ("swap", GATE_OTHER), (UP_OWN, 3), (BACK_LAST, 3), ("swap", BACK_OTHER),
    )
    swaps = {}
    for what, s in plan:
        if what == "swap":
            swaps[s] = swap(s)
        elif s < long:
            step(what, s)

    gate = swapped(GATE_OWN, swaps[GATE_OTHER])
    up = total(UP_OWN)
    back = jnp.concatenate([swapped(BACK_OWN, swaps[BACK_OTHER]), total(BACK_LAST)], axis=0)
    sig = jax.nn.sigmoid(gate)
    swished = gate * sig
    hidden = swished * up
    act[xl, z, 0:3] = hidden.astype(BF16)
    act[xl, z, 3:6] = (back * up * sig * (1.0 + gate * (1.0 - sig))).astype(BF16)
    act[xl, z, 6:9] = (back * swished).astype(BF16)
    sums = jnp.sum(jnp.sum(hidden * back, axis=0), axis=1, keepdims=True)
    diagonal = iota((slab, LANES), 0) == iota((slab, LANES), 1)
    rd[xl, z] = jnp.broadcast_to(
        jnp.sum(jnp.where(diagonal, sums, 0.0), axis=0, keepdims=True), (8, LANES)
    )

    own, other = half_of[True], half_of[False]
    comes, crossing = {}, {HID_OWN: [], GRAD_OWN: []}

    def ring_send(k, s, d):
        here, u0, n, far_way = GATHERS[k]
        where = at_z(s if d else -s)
        h, units = half_of[here], pl.ds(u0, n)
        both = [
            go_on(
                act.at[h, where, units], act.at[h, where, units], ag_send.at[k], ag_recv.at[k, d, s], toward[d],
                ("g%d" % k, act.at[0, pl.ds(0, nz - 1), units]),
            )
        ]
        if k == HID_OWN:
            both.append(go_on(rd.at[h, where], rd.at[h, where], rd_send.at[0], rd_recv.at[d, s], toward[d], ("rd", rd.at[0, pl.ds(0, nz - 1)])))
        comes[k, d] = both

    def cross(k, s, d):
        where = at_z(s if d else -s)
        u0, n = ACROSS[k]
        units = pl.ds(u0, n)
        j = int(k == GRAD_OWN)
        some = act.at[0, pl.ds(0, nz - 1), units]
        go_on(
            act.at[own, where, units], act.at[own, where, units], cross_send.at[j], cross_recv.at[j], partner,
            ("c%d" % k, some),
        )
        crossing[k] = [(some, cross_send.at[j], cross_recv.at[j])]
        if k == HID_OWN:
            some = rd.at[0, pl.ds(0, nz - 1)]
            go_on(rd.at[own, where], rd.at[own, where], cross_send.at[2], cross_recv.at[2], partner, ("cr", some))
            crossing[k].append((some, cross_send.at[2], cross_recv.at[2]))

    def ag_step(k, s):
        here, _, _, far_way = GATHERS[k]
        for d in range(2):
            length = long if d == far_way else short
            if s > length or (s == length and not here) or (s and (k, d) not in comes):
                continue
            if s:
                for c in comes[k, d]:
                    c.wait_recv()
            if s < length:
                ring_send(k, s, d)
            if s and here:
                cross(k, s, d)

    def ag_last(k):
        _, _, _, far_way = GATHERS[k]
        for d in range(2):
            if (k, d) in comes:
                for c in comes[k, d]:
                    c.wait_recv()

    firsts = {}

    def first(k, u0, n):
        units = pl.ds(u0, n)
        j = int(k == GRAD_OWN)
        firsts[k] = [
            go_on(act.at[own, z, units], act.at[own, z, units], first_send.at[j], first_recv.at[j], partner)
        ]
        if k == HID_OWN:
            firsts[k].append(go_on(rd.at[own, z], rd.at[own, z], first_send.at[2], first_recv.at[2], partner))

    first(HID_OWN, 0, 3)
    ag_step(HID_OWN, 0)
    first(GRAD_OWN, 3, 6)
    ag_step(GRAD_OWN, 0)
    for job in (
        (HID_OWN, 1), "hid", (HID_OTHER, 0), (GRAD_OWN, 1), "grad", (GRAD_OTHER, 0),
        (HID_OWN, 2), (HID_OTHER, 1), (GRAD_OWN, 2), (GRAD_OTHER, 1),
        (HID_OWN, 3), (HID_OTHER, 2), (GRAD_OWN, 3), (GRAD_OTHER, 2),
        (HID_OWN, 4), (HID_OTHER, 3), (GRAD_OWN, 4), (GRAD_OTHER, 3),
    ):
        if job in ("hid", "grad"):
            for c in firsts[HID_OWN if job == "hid" else GRAD_OWN]:
                c.wait_recv()
        elif job[1] <= long:
            ag_step(*job)
    ag_last(HID_OTHER)
    for c in crossing[HID_OWN]:
        all_of(*c).wait_recv()

    def whole(a):
        return jnp.concatenate(
            [act[h, :, 3 * a + u].reshape(rows, LANES) for h in range(2) for u in range(3)], axis=1
        )

    hid = whole(0)
    out_rows = dot(hid, dw[...]).astype(BF16)
    dots = jnp.concatenate([rd[0, j, 0:1, :] + rd[1, j, 0:1, :] for j in range(nz)], axis=0)
    dots = jnp.concatenate([dots, jnp.zeros((16 - nz, LANES), F32)], axis=0)
    high = dots.astype(BF16)
    low = (dots - high.astype(F32)).astype(BF16)
    spread = dot(grow, out_rows)
    spread = jnp.concatenate(
        [spread[:, :LANES] + dot(place_dot, high), spread[:, LANES : 2 * LANES] + dot(place_dot, low)]
        + ([spread[:, 2 * LANES :]] if feat > 2 * LANES else []),
        axis=1,
    )
    snd_o[...] = spread.reshape(n_expert, PAD, feat).astype(BF16)
    exchange(snd_o, rcv_o, 2)

    ag_last(GRAD_OTHER)
    for c in crossing[GRAD_OWN]:
        all_of(*c).wait_recv()
    g_grad, u_grad = whole(1), whole(2)
    in_rows = (dot(g_grad, gw[...], 1, 1) + dot(u_grad, uw[...], 1, 1)).astype(BF16)
    snd_i[...] = dot(grow, in_rows).reshape(n_expert, PAD, feat).astype(BF16)
    exchange(snd_i, rcv_i, 3)

    gg[...] = dot(xr[...], g_grad, 0, 0).astype(BF16)
    gu[...] = dot(xr[...], u_grad, 0, 0).astype(BF16)
    gd[...] = dot(hid, cr[...], 0, 0).astype(BF16)
    stores = []

    def store(src, dst):
        c = pltpu.make_async_copy(src, dst, out_sem.at[len(stores)])
        c.start()
        stores.append(c)

    store(gg, gg_hbm)
    store(gu, gu_hbm)
    store(gd, gd_hbm)
    for c in sent:
        c.wait_send()
    for ref, sem in waits.values():
        all_of(ref, sem, first_recv.at[0]).wait_send()
    exchange_all(snd, rcv, 0).wait_send()

    exchange_all(snd_o, rcv_o, 2).wait_recv()
    back_out = rcv_o[...].reshape(padded, feat)
    mixed[...] = (p[0] * dot(take[0], back_out) + p[1] * dot(take[1], back_out)).astype(BF16)
    lane = iota((toks, LANES), 1)
    start = (lax.rem(me, per_slab) * capacity).astype(F32)
    cols = []
    for k in range(2):
        found = dot(take_dot[k], back_out)
        picked = jnp.where(lane == start + pos_col[k], found[:, :LANES] + found[:, LANES : 2 * LANES], 0.0)
        cols.append(jnp.sum(picked, axis=1, keepdims=True) / p[k])
    groute[...] = jnp.concatenate(cols + [jnp.zeros((toks, toks - 2), F32)], axis=1).T[0:2, :]
    store(mixed, mixed_hbm)
    store(groute, groute_hbm)
    exchange_all(snd_i, rcv_i, 3).wait_recv()
    gtok[...] = dot(take[0] + take[1], rcv_i[...].reshape(padded, feat)).astype(BF16)
    store(gtok, gtok_hbm)
    exchange_all(snd_o, rcv_o, 2).wait_send()
    exchange_all(snd_i, rcv_i, 3).wait_send()
    for c in stores:
        c.wait()


def put_out(*refs):
    sem = refs[-1]
    n = (len(refs) - 1) // 3
    come = [pltpu.make_async_copy(refs[i], refs[2 * n + i], sem.at[0, i]) for i in range(n)]
    go = [pltpu.make_async_copy(refs[2 * n + i], refs[n + i], sem.at[1, i]) for i in range(n)]
    for c in come:
        c.start()
    for c, d in zip(come, go):
        c.wait()
        d.start()
    for d in go:
        d.wait()


def local(n_dp, n_expert, tokens, grad_out, expert_ids, route_weights, gate_weight, up_weight, down_weight):
    toks, feat = tokens.shape
    top = expert_ids.shape[1]
    hid = gate_weight.shape[2]
    nz = n_dp // 2
    capacity = max(2, 3 * toks * top // (2 * n_expert))
    rows = n_expert * capacity
    slab = rows // nz
    hop = max(1, nz // 2)
    hbm = pl.BlockSpec(memory_space=pltpu.HBM)
    wire = pltpu.VMEM((n_expert, PAD, feat), BF16)
    front = pltpu.VMEM((n_expert, 2 * feat // LANES * capacity // PAD, PAD, LANES), BF16)
    units = (9, slab, LANES)
    dma = pltpu.SemaphoreType.DMA
    shapes = (
        ((toks, feat), BF16),
        ((toks, feat), BF16),
        ((top, toks), F32),
        ((feat, hid), BF16),
        ((feat, hid), BF16),
        ((hid, feat), BF16),
    )
    out = pl.pallas_call(
        functools.partial(kernel, n_dp, n_expert, capacity),
        out_shape=tuple(jax.ShapeDtypeStruct(s, d) for s, d in shapes),
        in_specs=[hbm] * 7,
        out_specs=(hbm,) * 6,
        scratch_shapes=[
            pltpu.VMEM((toks, feat), BF16),
            pltpu.VMEM((toks, feat), BF16),
            pltpu.VMEM((top, toks), jnp.int32),
            pltpu.VMEM((top, toks), F32),
            pltpu.VMEM((feat, hid), BF16),
            pltpu.VMEM((feat, hid), BF16),
            pltpu.VMEM((hid, feat), BF16),
            *[front] * 2,
            *[wire] * 4,
            pltpu.VMEM((rows, feat), BF16),
            pltpu.VMEM((rows, feat), BF16),
            *[pltpu.VMEM(s, d) for s, d in shapes],
            pltpu.VMEM((2, nz, *units), BF16),
            pltpu.VMEM((2, 2, hop, *units), BF16),
            pltpu.VMEM((2, 2, hop, *units), BF16),
            pltpu.VMEM((nz, *units), BF16),
            pltpu.VMEM(units, BF16),
            pltpu.VMEM(units, BF16),
            pltpu.VMEM((2, nz, *units), BF16),
            pltpu.VMEM((2, nz, 8, LANES), F32),
            dma((7,)),
            dma((6,)),
            dma((8,)),
            dma((6,)),
            dma((6, 2, hop)),
            dma((2,)),
            dma((2, nz)),
            dma((2,)),
            dma((2,)),
            dma((4,)),
            dma((4, 2, hop)),
            dma((3,)),
            dma((3,)),
            dma((1,)),
            dma((2, hop)),
            dma((3,)),
            dma((3,)),
        ],
        compiler_params=pltpu.CompilerParams(
            collective_id=0, has_side_effects=True
        ),
        name="routed_layer",
    )(
        tokens, grad_out, expert_ids.T, route_weights.T,
        gate_weight.reshape(feat, hid), up_weight.reshape(feat, hid), down_weight.reshape(hid, feat),
    )
    mixed, gtok, groute, gg, gu, gd = pl.pallas_call(
        put_out,
        out_shape=tuple(jax.ShapeDtypeStruct(s, d) for s, d in shapes),
        in_specs=[hbm] * 6,
        out_specs=(hbm,) * 6,
        scratch_shapes=[pltpu.VMEM(s, d) for s, d in shapes] + [dma((2, 6))],
        name="put_out",
    )(*out)
    return mixed, gtok, groute.T, gg[None], gu[None], gd[None]


def solution(mesh):
    placed = (
        P("expert", "dp"),
        P("expert", "dp"),
        P("expert", None),
        P("expert", None),
        P("expert", "dp", None),
        P("expert", "dp", None),
        P("expert", None, "dp"),
    )
    return jax.shard_map(
        functools.partial(local, mesh.shape["dp"], mesh.shape["expert"]),
        mesh=mesh,
        in_specs=placed,
        out_specs=(
            P("expert", "dp"),
            P("expert", "dp"),
            P("expert", None),
            P("expert", "dp", None),
            P("expert", "dp", None),
            P("expert", None, "dp"),
        ),
        check_vma=False,
    )
```
